32 devices in a mesh: rep: 1, dp: 32 (over x, y, z, core).
Axes of the slice: x: 2, y: 2, z: 4, core: 2. Of those that a mesh axis runs over, the one named last changes fastest.
Arguments:
- x: bfloat16 [32, 2048, 1280], P(('rep', 'dp'))
- dy: bfloat16 [32, 2048, 1280], P(('rep', 'dp'))
- w_gate: bfloat16 [2, 1280, 3072], replicated
- w_up: bfloat16 [2, 1280, 3072], replicated
- w_down: bfloat16 [2, 3072, 1280], replicated
- m_w_gate: float32 [2, 1280, 3072], P(None, 'dp')
- m_w_up: float32 [2, 1280, 3072], P(None, 'dp')
- m_w_down: float32 [2, 3072, 1280], P(None, 'dp')
- v_w_gate: float32 [2, 1280, 3072], P(None, 'dp')
- v_w_up: float32 [2, 1280, 3072], P(None, 'dp')
- v_w_down: float32 [2, 3072, 1280], P(None, 'dp')
Outputs:
- output 1: bfloat16 [2, 1280, 3072], P('rep')
- output 2: bfloat16 [2, 1280, 3072], P('rep')
- output 3: bfloat16 [2, 3072, 1280], P('rep')
- output 4: float32 [2, 1280, 3072], P('rep', 'dp')
- output 5: float32 [2, 1280, 3072], P('rep', 'dp')
- output 6: float32 [2, 3072, 1280], P('rep', 'dp')
- output 7: float32 [2, 1280, 3072], P('rep', 'dp')
- output 8: float32 [2, 1280, 3072], P('rep', 'dp')
- output 9: float32 [2, 3072, 1280], P('rep', 'dp')
All inputs are finite; a program needn't handle non-finite values.
Results may differ from the reference program's by a relative error of at most 0.022.
Values are sent between devices in bfloat16 or wider.
A program may use at most 2 GiB of HBM per device.

```python
import jax
import jax.numpy as jnp
from jax import lax

SEQUENCES = 32
TOKENS = 2048
D = 1280
FF = 3072
LAYERS = 2
NAMES = ("w_gate", "w_up", "w_down")
SHAPES = {"w_gate": (LAYERS, D, FF), "w_up": (LAYERS, D, FF), "w_down": (LAYERS, FF, D)}


def bump(key, n, height):
    away = (jnp.arange(n, dtype=jnp.int32) - jax.random.randint(key, (), 0, n, jnp.int32)) % n
    return jnp.where(away < n // 8, height, 1.0)


def together(key, own, strength):
    shared = jax.random.normal(key, own.shape[1:], jnp.float32)
    return (own + strength * shared) * lax.rsqrt(1 + strength * strength)


def setup_inputs(seed: int = 0, part: int = 0) -> dict:
    kx, kdy, ka, kb, kz, kf, kh, kl, *keys = jax.random.split(jax.random.key(seed), 8 + 3 * len(NAMES))
    kx, kdy, ka, kb = (jax.random.fold_in(k, part) for k in (kx, kdy, ka, kb))
    kw, km, kv = (keys[i::3] for i in range(3))
    shape = (SEQUENCES, TOKENS, D)
    much_x, much_dy = jax.random.uniform(kz, (2,), jnp.float32, 0.0, 1.0)
    loud = 2.0 ** jax.random.uniform(jax.random.fold_in(kz, 1), (), jnp.float32, -1.0, 2.0)
    layers = 2.0 ** jax.random.uniform(kl, (LAYERS, 1, 1), jnp.float32, -1.0, 1.0)
    x = together(ka, jax.random.normal(kx, shape, jnp.float32), much_x) * bump(kf, D, 4.0)
    dy = together(kb, jax.random.normal(kdy, shape, jnp.float32), much_dy)
    drawn = {"x": x.astype(jnp.bfloat16), "dy": (loud * dy * (SEQUENCES * TOKENS) ** -0.5).astype(jnp.bfloat16)}
    for key, name in zip(kw, NAMES, strict=True):
        w = jax.random.normal(key, SHAPES[name], jnp.float32) * SHAPES[name][1] ** -0.5
        drawn[name] = (w * {"w_gate": 1.0, "w_up": bump(kh, FF, 4.0), "w_down": layers}[name]).astype(jnp.bfloat16)
    for key, name in zip(km, NAMES, strict=True):
        drawn[f"m_{name}"] = 0.1 * jax.random.normal(key, SHAPES[name], jnp.float32)
    for key, name in zip(kv, NAMES, strict=True):
        drawn[f"v_{name}"] = jax.random.uniform(key, SHAPES[name], jnp.float32, 0.005, 0.015)
    return drawn


def matmul(a, w):
    return jnp.dot(a, w, preferred_element_type=jnp.float32).astype(jnp.bfloat16)


def normed(h):
    wide = h.astype(jnp.float32)
    scale = lax.rsqrt(jnp.mean(wide**2, -1, keepdims=True) + 1e-6)
    return (wide * scale).astype(jnp.bfloat16)


def layer(h, w):
    a = normed(h)
    gate = jnp.dot(a, w["w_gate"], preferred_element_type=jnp.float32)
    up = jnp.dot(a, w["w_up"], preferred_element_type=jnp.float32)
    return h + matmul((jax.nn.silu(gate) * up).astype(jnp.bfloat16), w["w_down"])


def adamw(w, m, v, g):
    m = 0.9 * m + 0.1 * g
    v = 0.95 * v + 0.05 * g * g
    step = m * lax.rsqrt(v + 1e-8) + 0.1 * w
    return (w - 0.02 * step).astype(jnp.bfloat16), m, v


def clipped(gradients, sum_of_squares, count):
    factor = jnp.minimum(1.0, 0.5 * lax.rsqrt(sum_of_squares / count + 1e-30))
    return [g * factor for g in gradients]


def stack(weights, h):
    return lax.scan(lambda h, w: (layer(h, w), None), h, weights)[0]


def reference(x, dy, w_gate, w_up, w_down, m_w_gate, m_w_up, m_w_down, v_w_gate, v_w_up, v_w_down):
    weights = dict(zip(NAMES, (w_gate, w_up, w_down), strict=True))

    def take(so_far, sequence):
        h, by_y = sequence
        _, back = jax.vjp(lambda w: stack(w, h), weights)
        return jax.tree.map(lambda total, term: total + term.astype(jnp.float32), so_far, back(by_y)[0]), None

    none_yet = {name: jnp.zeros(w.shape, jnp.float32) for name, w in weights.items()}
    by_weights, _ = lax.scan(take, none_yet, (x, dy))
    gradients = [by_weights[name].astype(jnp.bfloat16).astype(jnp.float32) for name in NAMES]
    gradients = clipped(gradients, sum(jnp.sum(g * g) for g in gradients), sum(g.size for g in gradients))
    new = [
        adamw(w.astype(jnp.float32), m, v, g)
        for w, m, v, g in zip((w_gate, w_up, w_down), (m_w_gate, m_w_up, m_w_down), (v_w_gate, v_w_up, v_w_down), gradients, strict=True)
    ]
    return tuple(one[which] for which in range(3) for one in new)
```

```python
import functools

import jax
import jax.numpy as jnp
from jax import lax
from jax.experimental import pallas as pl
from jax.experimental.pallas import tpu as pltpu
from jax.sharding import PartitionSpec as P


NAMES = ("w_gate", "w_up", "w_down")


def matmul(a, w):
    return jnp.dot(a, w, preferred_element_type=jnp.float32).astype(jnp.bfloat16)


def normed(h):
    wide = h.astype(jnp.float32)
    scale = lax.rsqrt(jnp.mean(wide**2, -1, keepdims=True) + 1e-6)
    return (wide * scale).astype(jnp.bfloat16)


def layer(h, w):
    a = normed(h)
    gate = jnp.dot(a, w["w_gate"], preferred_element_type=jnp.float32)
    up = jnp.dot(a, w["w_up"], preferred_element_type=jnp.float32)
    return h + matmul((jax.nn.silu(gate) * up).astype(jnp.bfloat16), w["w_down"])


def adamw(w, m, v, g):
    m = 0.9 * m + 0.1 * g
    v = 0.95 * v + 0.05 * g * g
    step = m * lax.rsqrt(v + 1e-8) + 0.1 * w
    return (w - 0.02 * step).astype(jnp.bfloat16), m, v


def clipped(gradients, sum_of_squares, count):
    factor = jnp.minimum(1.0, 0.5 * lax.rsqrt(sum_of_squares / count + 1e-30))
    return [g * factor for g in gradients]


def stack(weights, h):
    for number in range(weights["w_gate"].shape[0]):
        h = layer(h, {name: w[number] for name, w in weights.items()})
    return h


MESHID = pl.DeviceIdType.MESH
def place():
    me = lax.axis_index("dp")
    return (me // 16) % 2, (me // 8) % 2, (me // 4) % 2, (me // 2) % 2, me % 2
MASK = (16, 8, 4, 2, 1)
def partner(pos, dim):
    me = lax.axis_index("dp")
    return me + MASK[dim] * (1 - 2 * pos[dim])
def dev(i): return {"rep": 0, "dp": i}
X, Y, ZH, ZL, C = range(5)
GATHER = ((ZH, ZL, Y, X, C), (ZH, X, ZL, Y, C), (ZH, Y, X, ZL, C))

def barrier(pos, dims):
    bar = pltpu.get_barrier_semaphore()
    for d in dims:
        pl.semaphore_signal(bar, inc=1, device_id=dev(partner(pos, d)), device_id_type=MESHID)
    pl.semaphore_wait(bar, len(dims))

def streams(sizes):
    groups = []
    for layer in (0, 1):
        for i in (0, 1, 2):
            for lo, parts in sizes[i]:
                g = []
                for colour, n in enumerate(parts):
                    g.append((i, layer, lo, n, colour)); lo += n
                groups.append(g)
    return groups

def gather_kernel(groups, own, out, send, recv, local):
    pos = place()
    for i in range(3):
        pass
    barrier(pos, range(5))
    me = tuple(pos)
    first = []
    for i in range(3):
        cp = pltpu.make_async_copy(own[i], out[i].at[(slice(None), *me)], local.at[i]); cp.start(); first.append(cp)
    def copy(n, s, phase):
        i, layer, lo, cols, colour = s
        order = GATHER[colour]
        done = order[:phase]
        d = order[phase]
        cs = pl.ds(lo, cols)
        if phase == 0:
            src = own[i].at[layer, :, cs]
        index = (layer, *(slice(None) if k in done else pos[k] for k in range(5)), slice(None), cs)
        dst = out[i].at[index]
        if phase: src = dst
        return pltpu.make_async_remote_copy(src_ref=src, dst_ref=dst, send_sem=send.at[n, phase], recv_sem=recv.at[n, phase],
                                            device_id=dev(partner(pos, d)), device_id_type=MESHID)
    started = []
    for k in range(len(groups) + 5):
        for g in range(len(groups)):
            phase = k - g
            if 0 <= phase <= 5:
                for j, s in enumerate(groups[g]):
                    n = 3 * g + j
                    if phase > 0: copy(n, s, phase - 1).wait_recv()
                    if phase == 1 and g == 0 and j == 0:
                        for cp in first: cp.wait()
                    if phase < 5:
                        c = copy(n, s, phase); c.start(); started.append(c)
    for c in started: c.wait_send()

SIZES = (((0, (1280, 1152, 640)),), ((0, (1280, 1152, 640)),), ((0, (512, 512, 256)),))
SIZES2 = (((0, (640, 640, 256)), (1536, (640, 512, 384))), ((0, (640, 640, 256)), (1536, (640, 512, 384))), ((0, (256, 256, 128)), (640, (256, 256, 128))))
def gather(own, sizes=SIZES):
    groups = streams(sizes)
    n = 3 * len(groups)
    def kernel(*refs):
        gather_kernel(groups, refs[:3], refs[3:6], *refs[6:])
    out = pl.pallas_call(kernel,
        out_shape=[jax.ShapeDtypeStruct((2, 2, 2, 2, 2, 2, *o.shape[1:]), o.dtype) for o in own],
        in_specs=[pl.BlockSpec(memory_space=pltpu.VMEM)] * 3, out_specs=[pl.BlockSpec(memory_space=pl.ANY)] * 3,
        scratch_shapes=[pltpu.SemaphoreType.DMA((n, 5)), pltpu.SemaphoreType.DMA((n, 5)), pltpu.SemaphoreType.DMA((3,))],
        compiler_params=pltpu.CompilerParams(collective_id=3, has_side_effects=True))(*own)
    return [o.reshape(2, -1, o.shape[-1]) for o in out]


def solution(mesh):
    def step(x, dy, *arrays):
        weights, m, v = (arrays[i : i + 3] for i in (0, 3, 6))
        x, dy = x[0], dy[0]
        _, back = jax.vjp(lambda w: stack(w, x), dict(zip(NAMES, weights, strict=True)))
        by_weights = back(dy)[0]
        gradients = [lax.psum_scatter(by_weights[name], "dp", scatter_dimension=1, tiled=True).astype(jnp.float32) for name in NAMES]
        squares = lax.psum(sum(jnp.sum(g * g) for g in gradients), "dp")
        gradients = clipped(gradients, squares, sum(w.size for w in weights))
        me = lax.axis_index("dp")
        own = [lax.dynamic_slice_in_dim(w, me * g.shape[1], g.shape[1], 1) for w, g in zip(weights, gradients)]
        new = [adamw(w.astype(jnp.float32), m, v, g) for w, m, v, g in zip(own, m, v, gradients, strict=True)]
        full = gather([one[0] for one in new])
        return (*full, *(one[1] for one in new), *(one[2] for one in new))

    data, whole, shard = P(("rep", "dp")), P(), P(None, "dp")
    return jax.shard_map(
        step,
        mesh=mesh,
        in_specs=(data, data, *[whole] * 3, *[shard] * 6),
        out_specs=(*[P("rep")] * 3, *[P("rep", "dp")] * 6),
        check_vma=False,
    )
```

```python
import functools

import jax
import jax.numpy as jnp
from jax import lax
from jax.experimental import pallas as pl
from jax.experimental.pallas import tpu as pltpu
from jax.sharding import PartitionSpec as P

FB = 256
MB = 1024
VMEM_LIMIT = 67_000_000
def nt(a, b): return lax.dot_general(a, b, (((1,), (1,)), ((), ())), preferred_element_type=jnp.float32)
def nn(a, b): return lax.dot_general(a, b, (((1,), (0,)), ((), ())), preferred_element_type=jnp.float32)
def one(shape): return pl.BlockSpec(shape, lambda *_: (0,) * len(shape), pipeline_mode=pl.Buffered(1))
def normed(h):
    wide = h.astype(jnp.float32)
    return (wide * lax.rsqrt(jnp.mean(wide**2, -1, keepdims=True) + 1e-6)).astype(jnp.bfloat16)
def silu_parts(g):
    s = 0.5 * jnp.tanh(0.5 * g) + 0.5
    return s, g * s

ROWS = 512
def f0_kernel(n, x, wg, wu, wd, g, u, actT, aT0, h1, a1, aT1, a, acc):
    j = pl.program_id(0)
    rows = x.shape[0]
    def block(r): return pl.ds(pl.multiple_of(r * ROWS, ROWS), ROWS)
    @pl.when(j == 0)
    def _():
        acc[...] = jnp.zeros_like(acc)
        @pl.loop(0, rows // ROWS)
        def _(r): a[block(r), :] = normed(x[block(r), :])
    @pl.when((j > 0) & (j <= rows // ROWS))
    def _(): aT0[...] = a[block(j - 1), :].T
    @pl.when(j < n)
    def _():
        for m in range(0, rows, MB):
            s = slice(m, m + MB)
            gg = nn(a[s, :], wg[0]); g[0, s, :] = gg
            uu = nn(a[s, :], wu[0]); u[0, s, :] = uu
            act = (silu_parts(gg)[1] * uu).astype(jnp.bfloat16)
            actT[:, s] = act.T
            acc[s, :] += nn(act, wd[0])
    @pl.when(j >= n)
    def _():
        s = block(j - n)
        h = x[s, :] + acc[s, :].astype(jnp.bfloat16)
        h1[...] = h
        b = normed(h)
        a1[...] = b
        aT1[...] = b.T
def f0_call(x, wg, wu, wd, layer=0):
    t, d = x.shape; ff = wg.shape[2]; n = ff // FB; k = t // ROWS
    bf, f32 = jnp.bfloat16, jnp.float32
    cur = lambda j: jnp.minimum(j, n - 1)
    end = lambda j: jnp.maximum(j - n, 0)
    return pl.pallas_call(functools.partial(f0_kernel, n), grid=(n + k,),
        in_specs=[one((t, d)), pl.BlockSpec((1, d, FB), lambda j: (layer, 0, cur(j))), pl.BlockSpec((1, d, FB), lambda j: (layer, 0, cur(j))),
                  pl.BlockSpec((1, FB, d), lambda j: (layer, cur(j), 0))],
        out_specs=[pl.BlockSpec((1, t, FB), lambda j: (cur(j), 0, 0)), pl.BlockSpec((1, t, FB), lambda j: (cur(j), 0, 0)), pl.BlockSpec((FB, t), lambda j: (cur(j), 0)),
                   pl.BlockSpec((d, ROWS), lambda j: (0, jnp.clip(j - 1, 0, k - 1))),
                   pl.BlockSpec((ROWS, d), lambda j: (end(j), 0)), pl.BlockSpec((ROWS, d), lambda j: (end(j), 0)), pl.BlockSpec((d, ROWS), lambda j: (0, end(j)))],
        out_shape=[jax.ShapeDtypeStruct((n, t, FB), f32)] * 2 + [jax.ShapeDtypeStruct((ff, t), bf), jax.ShapeDtypeStruct((d, t), bf),
                   jax.ShapeDtypeStruct((t, d), bf), jax.ShapeDtypeStruct((t, d), bf), jax.ShapeDtypeStruct((d, t), bf)],
        scratch_shapes=[pltpu.VMEM((t, d), bf), pltpu.VMEM((t, d), f32)],
        compiler_params=pltpu.CompilerParams(vmem_limit_bytes=VMEM_LIMIT))(x, wg, wu, wd)
def f1_kernel(a, dy, wg, wu, g, u, dwd, actT):
    for m in range(0, a.shape[0], MB):
        s = slice(m, m + MB)
        gg = nn(a[s, :], wg[0]); g[0, s, :] = gg
        uu = nn(a[s, :], wu[0]); u[0, s, :] = uu
        actT[:, s] = (silu_parts(gg)[1] * uu).astype(jnp.bfloat16).T
    dwd[...] = nn(actT[...], dy[...]).astype(jnp.bfloat16)
def f1_call(a, dy, wg, wu, layer=1):
    t, d = a.shape; ff = wg.shape[2]; n = ff // FB
    bf, f32 = jnp.bfloat16, jnp.float32
    return pl.pallas_call(f1_kernel, grid=(n,),
        in_specs=[one((t, d)), one((t, d)), pl.BlockSpec((1, d, FB), lambda j: (layer, 0, j)), pl.BlockSpec((1, d, FB), lambda j: (layer, 0, j))],
        out_specs=[pl.BlockSpec((1, t, FB), lambda j: (j, 0, 0)), pl.BlockSpec((1, t, FB), lambda j: (j, 0, 0)), pl.BlockSpec((FB, d), lambda j: (j, 0))],
        out_shape=[jax.ShapeDtypeStruct((n, t, FB), f32)] * 2 + [jax.ShapeDtypeStruct((ff, d), bf)],
        scratch_shapes=[pltpu.VMEM((FB, t), bf)],
        compiler_params=pltpu.CompilerParams(vmem_limit_bytes=VMEM_LIMIT))(a, dy, wg, wu)


MESHID = pl.DeviceIdType.MESH
def place():
    me = lax.axis_index("dp")
    return (me // 16) % 2, (me // 8) % 2, (me // 4) % 2, (me // 2) % 2, me % 2
MASK = (16, 8, 4, 2, 1)
def partner(pos, dim):
    me = lax.axis_index("dp")
    return me + MASK[dim] * (1 - 2 * pos[dim])
def dev(i): return {"rep": 0, "dp": i}
X, Y, ZH, ZL, C = range(5)
LAG = 2
GATHER = ((ZH, ZL, Y, X, C), (ZH, X, ZL, Y, C), (ZH, Y, X, ZL, C))

def barrier(pos, dims):
    bar = pltpu.get_barrier_semaphore()
    for d in dims:
        pl.semaphore_signal(bar, inc=1, device_id=dev(partner(pos, d)), device_id_type=MESHID)
    pl.semaphore_wait(bar, len(dims))

def streams(sizes):
    groups = []
    for layer in (0, 1):
        for i in (0, 1, 2):
            for lo, parts in sizes[i]:
                g = []
                for colour, n in enumerate(parts):
                    g.append((i, layer, lo, n, colour)); lo += n
                groups.append(g)
    return groups

def gather_kernel(groups, own, out, send, recv, local):
    pos = place()
    barrier(pos, range(5))
    me = tuple(pos)
    first = []
    for i in range(3):
        cp = pltpu.make_async_copy(own[i], out[i].at[(slice(None), *me)], local.at[i]); cp.start(); first.append(cp)
    def copy(n, s, phase):
        i, layer, lo, cols, colour = s
        order = GATHER[colour]
        done = order[:phase]
        d = order[phase]
        cs = pl.ds(lo, cols)
        if phase == 0:
            src = own[i].at[layer, :, cs]
        index = (layer, *(slice(None) if k in done else pos[k] for k in range(5)), slice(None), cs)
        dst = out[i].at[index]
        if phase: src = dst
        return pltpu.make_async_remote_copy(src_ref=src, dst_ref=dst, send_sem=send.at[n, phase], recv_sem=recv.at[n, phase],
                                            device_id=dev(partner(pos, d)), device_id_type=MESHID)
    started = []
    for k in range(len(groups) + 5 * LAG):
        for g in range(len(groups)):
            phase, odd = divmod(k - g, LAG)
            if 0 <= phase <= 5 and not odd:
                for j, s in enumerate(groups[g]):
                    n = 3 * g + j
                    if phase > 0: copy(n, s, phase - 1).wait_recv()
                    if phase == 1 and g == 0 and j == 0:
                        for cp in first: cp.wait()
                    if phase < 5:
                        c = copy(n, s, phase); c.start(); started.append(c)
    for c in started: c.wait_send()

WIDE = tuple((lo, (384, 384, 256)) for lo in (0, 1024, 2048))
NARROW = tuple((lo, (256, 256, 128)) for lo in (0, 640))
SIZES = (WIDE, WIDE, NARROW)
def gather(own, sizes=SIZES):
    groups = streams(sizes)
    n = 3 * len(groups)
    def kernel(*refs):
        gather_kernel(groups, refs[:3], refs[3:6], *refs[6:])
    out = pl.pallas_call(kernel,
        out_shape=[jax.ShapeDtypeStruct((2, 2, 2, 2, 2, 2, *o.shape[1:]), o.dtype) for o in own],
        in_specs=[pl.BlockSpec(memory_space=pltpu.VMEM)] * 3, out_specs=[pl.BlockSpec(memory_space=pl.ANY)] * 3,
        scratch_shapes=[pltpu.SemaphoreType.DMA((n, 5)), pltpu.SemaphoreType.DMA((n, 5)), pltpu.SemaphoreType.DMA((3,))],
        compiler_params=pltpu.CompilerParams(vmem_limit_bytes=20_000_000, collective_id=3, has_side_effects=True))(*own)
    return [o.reshape(2, -1, o.shape[-1]) for o in out]


ORDER = ((X, Y, ZL), (Y, ZL, X), (ZL, X, Y))
AFTER = (1, 3, 5, 7, 9)
DRAIN = AFTER[-1]

def two(q): return lax.rem(q, 2)
def four(q): return lax.rem(q, 4)
def dmas(*n): return pltpu.SemaphoreType.DMA(n)

class Stream:
    def __init__(self, half, lanes, cuts, count, first):
        self.half, self.lanes, self.cuts, self.count, self.first = half, lanes, cuts, count, first
    def scratch(self):
        r, n, bf = 2 * self.half, self.lanes, jnp.bfloat16
        rows = [b - a for a, b in zip(self.cuts, self.cuts[1:])]
        shapes = [pltpu.VMEM((2, 8, r, n), bf), pltpu.VMEM((2, 8, r, n), bf)]
        for rc in rows:
            for k in (8, 4, 2): shapes += [pltpu.VMEM((4, k, rc, n), bf), pltpu.VMEM((4, k // 2, rc, n), bf)]
        shapes += [pltpu.VMEM((4, r, n), jnp.float32), pltpu.VMEM((4, self.half, n), bf), pltpu.VMEM((4, self.half, n), bf)]
        shapes += [dmas(2), dmas(2), dmas(3, 3, 4), dmas(3, 3, 4),
                   dmas(4), dmas(4)]
        return shapes
    def bind(self, refs, pos, squares, store):
        self.pos, self.squares, self.store = pos, squares, store
        self.made, self.got = refs[0], refs[1]
        self.colours = [refs[2 + 6 * k : 8 + 6 * k] for k in range(3)]
        self.last, self.zsend, self.zgot, self.cs, self.cr, self.ps, self.pr, self.zs, self.zr = refs[20:]
        return self
    def core_copy(self, q):
        slot = two(q)
        return pltpu.make_async_remote_copy(src_ref=self.made.at[1 - self.pos[C]], dst_ref=self.got.at[slot], send_sem=self.cs.at[slot], recv_sem=self.cr.at[slot],
                                            device_id=dev(partner(self.pos, C)), device_id_type=MESHID)
    def chip_copy(self, colour, phase, q):
        slot = four(q)
        n = 8 >> phase
        d = ORDER[colour][phase]
        src = self.colours[colour][2 * phase].at[slot, pl.ds((1 - self.pos[d]) * (n // 2), n // 2)]
        dst = self.colours[colour][2 * phase + 1].at[slot]
        return pltpu.make_async_remote_copy(src_ref=src, dst_ref=dst, send_sem=self.ps.at[phase, colour, slot], recv_sem=self.pr.at[phase, colour, slot],
                                            device_id=dev(partner(self.pos, d)), device_id_type=MESHID)
    def z_copy(self, q):
        slot = four(q)
        return pltpu.make_async_remote_copy(src_ref=self.zsend.at[slot], dst_ref=self.zgot.at[slot], send_sem=self.zs.at[slot], recv_sem=self.zr.at[slot],
                                            device_id=dev(partner(self.pos, ZH)), device_id_type=MESHID)
    def send(self, t):
        q = t - self.first
        @pl.when((q >= 0) & (q < self.count))
        def _(): self.core_copy(q).start()
    def when(self, t, p, body):
        q = t - self.first - AFTER[p]
        @pl.when((q >= 0) & (q < self.count))
        def _(): body(q)
    def advance(self, t, stage):
        pos, f32, bf = self.pos, jnp.float32, jnp.bfloat16
        def finish(q):
            slot = four(q)
            self.z_copy(q).wait()
            keep = self.last[slot, pl.ds(pl.multiple_of(pos[ZH] * self.half, 8), self.half), :]
            total = (keep + self.zgot[slot].astype(f32)).astype(bf)
            self.store(q, total)
            square = total.astype(f32) ** 2
            square = sum(square[:, k : k + 128] for k in range(0, self.lanes, 128))
            self.squares[...] += sum(square[k : k + 8] for k in range(0, self.half, 8))
        def third(q):
            slot = from_ = four(q)
            for k in range(3):
                self.chip_copy(k, 2, q).wait()
                a, b = self.cuts[k], self.cuts[k + 1]
                s, r = self.colours[k][4:6]
                self.last[slot, a:b, :] = s[from_, pos[ORDER[k][2]]].astype(f32) + r[from_, 0].astype(f32)
            self.zsend[slot] = self.last[slot, pl.ds(pl.multiple_of((1 - pos[ZH]) * self.half, 8), self.half), :].astype(bf)
            self.z_copy(q).start()
        def second(q):
            slot = four(q)
            for k in range(3):
                self.chip_copy(k, 1, q).wait()
                s, r, s2 = self.colours[k][2:5]
                for i in range(2):
                    s2[slot, i] = (s[slot, 2 * pos[ORDER[k][1]] + i].astype(f32) + r[slot, i].astype(f32)).astype(bf)
                self.chip_copy(k, 2, q).start()
        def first(q):
            slot = into = four(q)
            for k in range(3):
                self.chip_copy(k, 0, q).wait()
                s, r, s2 = self.colours[k][:3]
                for i in range(4):
                    s2[into, i] = (s[slot, 4 * pos[ORDER[k][0]] + i].astype(f32) + r[slot, i].astype(f32)).astype(bf)
                self.chip_copy(k, 1, q).start()
        def cores(q):
            slot, into = two(q), four(q)
            self.core_copy(q).wait()
            @pl.loop(0, 8, unroll=4)
            def _(b):
                bits = {X: b // 4, Y: (b // 2) % 2, ZL: b % 2}
                total = (self.made[pos[C], b].astype(f32) + self.got[slot, b].astype(f32)).astype(bf)
                for k in range(3):
                    d = ORDER[k]
                    self.colours[k][0][into, 4 * bits[d[0]] + 2 * bits[d[1]] + bits[d[2]]] = total[self.cuts[k] : self.cuts[k + 1]]
            for k in range(3): self.chip_copy(k, 0, q).start()
        self.when(t, stage, (cores, first, second, third, finish)[stage])
    def put(self, whole, x=None):
        h = self.half
        for c in range(2):
            for b in range(8 if x is None else 4):
                r = ((b // 2) * 8 + (b % 2) * 2 + c) * h
                parts = [whole[r + zh * 4 * h : r + (zh * 4 + 1) * h, :] for zh in range(2)]
                self.made[c, b + 4 * (x or 0)] = jnp.concatenate(parts, 0).astype(jnp.bfloat16)

def advance(t, *streams):
    for stage in (4, 3, 2, 1, 0):
        for one_of in streams: one_of.advance(t, stage)

def elem(dact, g, u):
    dact = dact.astype(jnp.bfloat16).astype(jnp.float32)
    s, silu = silu_parts(g)
    return (dact * u * (s * (1 + g - silu))).astype(jnp.bfloat16), (dact * silu).astype(jnp.bfloat16)

NROWS = 256
TILE = (8, 128)
def before_gates(dy, wd, g, u, dgu):
    for m in range(0, dy.shape[0], EB):
        s = slice(m, m + EB)
        dgu[s, :FB], dgu[s, FB:] = elem(nt(dy[s, :], wd[0]), g[0, s, :], u[0, s, :])

EB, AB = 256, 512
CUT40, CUT96 = (0, 32, 64, 80), (0, 80, 144, 192)

def store_in(out, width):
    def store(q, total): out[:, pl.ds(pl.multiple_of(q * width, width), width)] = total
    return store
def store_pair(gate, up):
    def store(q, total):
        s = pl.ds(pl.multiple_of(q * FB, FB), FB)
        gate[:, s] = total[:, :FB]
        up[:, s] = total[:, FB:]
    return store
def b1_kernel(n, aT, dy, h1, g, u, wg, wu, wd, dwd, dh, out_g, out_u, out_d, squares, dgu, acc, tmp, *refs):
    t = pl.program_id(0)
    pos = place()
    G = Stream(40, 2 * FB, CUT40, n, 0); Dn = Stream(96, 128, CUT96, n - 2, 0)
    ng = len(G.scratch())
    G.bind(refs[:ng], pos, squares, store_pair(out_g, out_u)); Dn.bind(refs[ng:], pos, squares, store_in(out_d, 128))
    @pl.when(t == 0)
    def _():
        barrier(pos, range(5))
        acc[...] = jnp.zeros_like(acc)
        squares[...] = jnp.zeros_like(squares)
    @pl.when(t < n)
    def _():
        before_gates(dy, wd, g, u, dgu)
    advance(t, Dn, G)
    @pl.when(t < Dn.count)
    def _(): Dn.put(dwd)
    Dn.send(t)
    @pl.when(t < n)
    def _():
        tmp[...] = nn(aT[...], dgu[...])
        G.put(tmp)
        for m in range(0, dy.shape[0], AB):
            s = slice(m, m + AB)
            acc[s, :] += nt(dgu[s, :FB], wg[0]) + nt(dgu[s, FB:], wu[0])
    G.send(t)
    @pl.when((t >= n) & (t < n + dy.shape[0] // NROWS))
    def _():
        s = pl.ds(pl.multiple_of((t - n) * NROWS, NROWS), NROWS)
        wide, da = h1[...].astype(jnp.float32), acc[s, :].astype(jnp.bfloat16).astype(jnp.float32)
        scale = lax.rsqrt(jnp.mean(wide**2, -1, keepdims=True) + 1e-6)
        dwide = da * scale - wide * (scale * scale * scale * jnp.mean(da * wide, -1, keepdims=True))
        dh[...] = dy[s, :] + dwide.astype(jnp.bfloat16)

def b1_call(aT, dy, h1, g, u, wg, wu, wd, dwd, layer=1):
    d, tk = aT.shape; ff = wg.shape[2]; n = ff // FB; k = tk // NROWS
    G = Stream(40, 2 * FB, CUT40, n, 0); Dn = Stream(96, 128, CUT96, n - 2, 0)
    bf, f32 = jnp.bfloat16, jnp.float32
    own = [(G.half, ff), (G.half, ff), (Dn.half, d)]
    cur = lambda j: jnp.minimum(j, n - 1)
    end = lambda j: jnp.clip(j - n, 0, k - 1)
    return pl.pallas_call(functools.partial(b1_kernel, n), grid=(n + DRAIN,),
        in_specs=[one((d, tk)), one((tk, d)), pl.BlockSpec((NROWS, d), lambda j: (end(j), 0)),
                  pl.BlockSpec((1, tk, FB), lambda j: (cur(j), 0, 0)), pl.BlockSpec((1, tk, FB), lambda j: (cur(j), 0, 0)),
                  pl.BlockSpec((1, d, FB), lambda j: (layer, 0, cur(j))), pl.BlockSpec((1, d, FB), lambda j: (layer, 0, cur(j))), pl.BlockSpec((1, FB, d), lambda j: (layer, cur(j), 0)),
                  pl.BlockSpec((ff, 128), lambda j: (0, jnp.minimum(j, n - 3)))],
        out_specs=[pl.BlockSpec((NROWS, d), lambda j: (end(j), 0)), *map(one, own), one(TILE)],
        out_shape=[jax.ShapeDtypeStruct((tk, d), bf), *[jax.ShapeDtypeStruct(o, bf) for o in own], jax.ShapeDtypeStruct(TILE, f32)],
        scratch_shapes=[pltpu.VMEM((tk, 2 * FB), bf), pltpu.VMEM((tk, d), f32), pltpu.VMEM((d, 2 * FB), f32)] + G.scratch() + Dn.scratch(),
        compiler_params=pltpu.CompilerParams(vmem_limit_bytes=VMEM_LIMIT, collective_id=1, has_side_effects=True))(aT, dy, h1, g, u, wg, wu, wd, dwd)

def others(dims):
    me, pos = lax.axis_index("dp"), place()
    for which in range(1, 1 << len(dims)):
        yield me + sum(MASK[d] * (1 - 2 * pos[d]) for k, d in enumerate(dims) if which >> k & 1)
def greet(groups):
    bar = pltpu.get_barrier_semaphore()
    count = 0
    for dims in groups:
        for other in others(dims):
            pl.semaphore_signal(bar, inc=1, device_id=dev(other), device_id_type=MESHID)
            count += 1
    pl.semaphore_wait(bar, count)
def everyone(value, got, send, recv, dims, first):
    pos = place()
    n = 1 << len(dims)
    mine = sum(pos[d] << k for k, d in enumerate(dims))
    copies = []
    for k, other in enumerate(others(dims)):
        copies.append(pltpu.make_async_remote_copy(src_ref=value, dst_ref=got.at[first + mine], send_sem=send.at[first + k], recv_sem=recv.at[first + k],
                                                   device_id=dev(other), device_id_type=MESHID))
    for c in copies: c.start()
    got[first + mine] = value[...]
    for c in copies: c.wait()
    value[...] = sum(got[first + k] for k in range(n))

def b0_kernel(n, nb, count, aT, dh, wd, squares1, g_all, u_all, actT, out_g, out_u, out_d, factor, g, u, gsem, tmp, dgu, act, asem, squares, sgot, ssend, srecv, *refs):
    t = pl.program_id(0)
    pos = place()
    G = Stream(40, 2 * FB, CUT40, n, 0); Dn = Stream(96, FB, CUT96, nb, 0)
    ng = len(G.scratch())
    G.bind(refs[:ng], pos, squares, store_pair(out_g, out_u)); Dn.bind(refs[ng:], pos, squares, store_in(out_d, FB))
    rows = act.shape[1]
    def fetch(b): return pltpu.make_async_copy(actT.at[b * rows : (b + 1) * rows, :], act.at[b], asem.at[b])
    def saved(j): return [pltpu.make_async_copy(a.at[j], b.at[0], gsem.at[k]) for k, (a, b) in enumerate(((g_all, g), (u_all, u)))]
    @pl.when(t == 0)
    def _():
        for b in range(4): fetch(b).start()
        for c in saved(0): c.start()
        greet(((X, Y, C), (ZH, ZL)))
        squares[...] = squares1[...]
    advance(t, Dn)
    @pl.when(t < nb)
    def _():
        columns = pl.ds(pl.multiple_of(t * FB, FB), FB)
        for xy in range(4):
            @pl.when(t == 0)
            def _(): fetch(xy).wait()
            for zh in range(2):
                value = nn(act[xy, zh * rows // 2 : (zh + 1) * rows // 2, :], dh[:, columns])
                for zl in range(2):
                    for c in range(2):
                        r = (zl * 2 + c) * 96
                        Dn.made[c, xy * 2 + zl, zh * 96 : zh * 96 + 96, :] = value[r : r + 96].astype(jnp.bfloat16)
    Dn.send(t)
    @pl.when(t < n)
    def _():
        for c in saved(t): c.wait()
        before_gates(dh, wd, g, u, dgu)
    @pl.when(t < n - 1)
    def _():
        for c in saved(t + 1): c.start()
    advance(t, G)
    @pl.when(t < n)
    def _():
        half = aT.shape[0] // 2
        for x in range(2):
            tmp[...] = nn(aT[x * half : (x + 1) * half, :], dgu[...])
            G.put(tmp, x)
    G.send(t)
    @pl.when(t == n + DRAIN - 1)
    def _():
        everyone(squares, sgot, ssend, srecv, (X, Y, C), 0)
        everyone(squares, sgot, ssend, srecv, (ZH, ZL), 8)
        total = jnp.sum(jnp.sum(squares[...], 1, keepdims=True), 0, keepdims=True)
        factor[...] = jnp.broadcast_to(jnp.minimum(1.0, 0.5 * lax.rsqrt(total / count + 1e-30)), factor.shape)

def b0_call(aT, dh, actT, g, u, wd, squares1, count, layer=0):
    d, tk = aT.shape; ff = wd.shape[1]; n = ff // FB; nb = d // FB
    G = Stream(40, 2 * FB, CUT40, n, 0); Dn = Stream(96, FB, CUT96, nb, 0)
    bf, f32 = jnp.bfloat16, jnp.float32
    own = [(G.half, ff), (G.half, ff), (Dn.half, d)]
    cur = lambda j: jnp.minimum(j, n - 1)
    return pl.pallas_call(functools.partial(b0_kernel, n, nb, count), grid=(n + DRAIN,),
        in_specs=[one((d, tk)), one((tk, d)),
                  pl.BlockSpec((1, FB, d), lambda j: (layer, cur(j), 0)), one(TILE), *[pl.BlockSpec(memory_space=pl.ANY)] * 3],
        out_specs=[*map(one, own), one(TILE)],
        out_shape=[*[jax.ShapeDtypeStruct(o, bf) for o in own], jax.ShapeDtypeStruct(TILE, f32)],
        scratch_shapes=[*[pltpu.VMEM((1, tk, FB), f32)] * 2, dmas(2), pltpu.VMEM((d // 2, 2 * FB), f32), pltpu.VMEM((tk, 2 * FB), bf), pltpu.VMEM((4, ff // 4, tk), bf), dmas(4),
                        pltpu.VMEM(TILE, f32), pltpu.VMEM((12, *TILE), f32), dmas(12), dmas(12)] + G.scratch() + Dn.scratch(),
        compiler_params=pltpu.CompilerParams(vmem_limit_bytes=VMEM_LIMIT, collective_id=2, has_side_effects=True))(aT, dh, wd, squares1, g, u, actT)


def adamw(w, m, v, g):
    m = 0.9 * m + 0.1 * g
    v = 0.95 * v + 0.05 * g * g
    step = m * lax.rsqrt(v + 1e-8) + 0.1 * w
    return (w - 0.02 * step).astype(jnp.bfloat16), m, v


def solution(mesh):
    def step(x, dy, *arrays):
        weights, m, v = (arrays[i : i + 3] for i in (0, 3, 6))
        x, dy = x[0], dy[0]
        wg, wu, wd = weights
        g0, u0, actT0, aT0, h1, a1, aT1 = f0_call(x, wg, wu, wd)
        g1, u1, dwd1 = f1_call(a1, dy, wg, wu)
        dh1, *of1, squares1 = b1_call(aT1, dy, h1, g1, u1, wg, wu, wd, dwd1)
        *of0, factor = b0_call(aT0, dh1, actT0, g0, u0, wd, squares1, sum(w.size for w in weights))
        gradients = [jnp.stack([a, b]).astype(jnp.float32) for a, b in zip(of0, of1)]
        factor = factor[0, 0]
        me = lax.axis_index("dp")
        own = [lax.dynamic_slice_in_dim(w, me * g.shape[1], g.shape[1], 1) for w, g in zip(weights, gradients)]
        new = [adamw(w.astype(jnp.float32), m, v, g * factor) for w, m, v, g in zip(own, m, v, gradients, strict=True)]
        full = gather([one[0] for one in new])
        return (*full, *(one[1] for one in new), *(one[2] for one in new))

    data, whole, shard = P(("rep", "dp")), P(), P(None, "dp")
    return jax.shard_map(
        step,
        mesh=mesh,
        in_specs=(data, data, *[whole] * 3, *[shard] * 6),
        out_specs=(*[P("rep")] * 3, *[P("rep", "dp")] * 6),
        check_vma=False,
    )
```
